16 devices in a mesh: tp: 2 (over z), pp: 8 (over y, x, core).
Axes of the slice: x: 2, y: 2, z: 2, core: 2. Of those that a mesh axis runs over, the one named last changes fastest.
Arguments:
- x_micro: bfloat16 [48, 1, 128, 2048], replicated
- ln1_gain: bfloat16 [8, 2048], P('pp')
- ln1_bias: bfloat16 [8, 2048], P('pp')
- w_qkv: bfloat16 [8, 2048, 16, 384], P('pp', None, 'tp')
- b_qkv: bfloat16 [8, 16, 384], P('pp', 'tp')
- w_dense: bfloat16 [8, 16, 128, 2048], P('pp', 'tp')
- b_dense: bfloat16 [8, 2048], P('pp')
- ln2_gain: bfloat16 [8, 2048], P('pp')
- ln2_bias: bfloat16 [8, 2048], P('pp')
- w_up: bfloat16 [8, 2048, 8192], P('pp', None, 'tp')
- b_up: bfloat16 [8, 8192], P('pp', 'tp')
- w_down: bfloat16 [8, 8192, 2048], P('pp', 'tp')
- b_down: bfloat16 [8, 2048], P('pp')
Outputs:
- output: bfloat16 [48, 1, 128, 2048], replicated
All inputs are finite; a program needn't handle non-finite values.
Results may differ from the reference program's by a relative error of at most 0.02.
Values are sent between devices in bfloat16 or wider.
A program may use at most 1 GiB of HBM per device.

```python
import jax
import jax.numpy as jnp
from jax import lax

D = 2048
HEADS = 16
LAYERS = 8
MICRO = 48
BATCH = 1
SEQ = 128
HEAD = D // HEADS
FFN = 4 * D
ROT = HEAD // 4


def setup_inputs(seed: int = 0) -> dict:
    key_list = jax.random.split(jax.random.key(seed), 13)

    def normal(sub_key, shape, scale):
        return jax.random.normal(sub_key, shape, jnp.float32) * scale

    qk_scale = jnp.concatenate([jnp.full((2 * HEAD,), 1.6, jnp.float32), jnp.ones((HEAD,), jnp.float32)])
    return {
        "x_micro": normal(key_list[0], (MICRO, BATCH, SEQ, D), 1.0).astype(jnp.bfloat16),
        "ln1_gain": (1.0 + normal(key_list[1], (LAYERS, D), 0.3)).astype(jnp.bfloat16),
        "ln1_bias": normal(key_list[2], (LAYERS, D), 0.3).astype(jnp.bfloat16),
        "w_qkv": (normal(key_list[3], (LAYERS, D, HEADS, 3 * HEAD), D ** -0.5) * qk_scale).astype(jnp.bfloat16),
        "b_qkv": normal(key_list[4], (LAYERS, HEADS, 3 * HEAD), 0.3).astype(jnp.bfloat16),
        "w_dense": normal(key_list[5], (LAYERS, HEADS, HEAD, D), D ** -0.5).astype(jnp.bfloat16),
        "b_dense": normal(key_list[6], (LAYERS, D), 0.3).astype(jnp.bfloat16),
        "ln2_gain": (1.0 + normal(key_list[7], (LAYERS, D), 0.3)).astype(jnp.bfloat16),
        "ln2_bias": normal(key_list[8], (LAYERS, D), 0.3).astype(jnp.bfloat16),
        "w_up": normal(key_list[9], (LAYERS, D, FFN), D ** -0.5).astype(jnp.bfloat16),
        "b_up": normal(key_list[10], (LAYERS, FFN), 0.3).astype(jnp.bfloat16),
        "w_down": normal(key_list[11], (LAYERS, FFN, D), FFN ** -0.5).astype(jnp.bfloat16),
        "b_down": normal(key_list[12], (LAYERS, D), 0.3).astype(jnp.bfloat16),
    }


def layer_norm(x_act, gain, bias):
    x_f32 = x_act.astype(jnp.float32)
    centered = x_f32 - jnp.mean(x_f32, axis=-1, keepdims=True)
    spread = jnp.mean(centered * centered, axis=-1, keepdims=True)
    normed = centered * lax.rsqrt(spread + 1e-5)
    return (normed * gain.astype(jnp.float32) + bias.astype(jnp.float32)).astype(jnp.bfloat16)


def rotary_tables():
    inv_freq = 1.0 / (10000.0 ** (jnp.arange(0, ROT, 2).astype(jnp.float32) / ROT))
    angles = jnp.arange(SEQ).astype(jnp.float32)[:, None] * inv_freq[None, :]
    angles = jnp.concatenate([angles, angles], axis=-1)
    return jnp.cos(angles), jnp.sin(angles)


def apply_rotary(heads_in, cos_tab, sin_tab):
    half_rot = ROT // 2
    rot_part = heads_in[..., :ROT].astype(jnp.float32)
    rotated = jnp.concatenate([-rot_part[..., half_rot:], rot_part[..., :half_rot]], axis=-1)
    mixed = rot_part * cos_tab[:, None, :] + rotated * sin_tab[:, None, :]
    return jnp.concatenate([mixed.astype(jnp.bfloat16), heads_in[..., ROT:]], axis=-1)


def neox_row(x_row, layer, cos_tab, sin_tab):
    ln_attn = layer_norm(x_row, layer["ln1_gain"], layer["ln1_bias"])
    qkv_proj = jnp.dot(ln_attn, layer["w_qkv"].reshape(D, HEADS * 3 * HEAD), preferred_element_type=jnp.float32)
    qkv_proj = (qkv_proj.reshape(SEQ, HEADS, 3 * HEAD) + layer["b_qkv"].astype(jnp.float32)).astype(jnp.bfloat16)
    query = apply_rotary(qkv_proj[..., :HEAD], cos_tab, sin_tab)
    key_rot = apply_rotary(qkv_proj[..., HEAD:2 * HEAD], cos_tab, sin_tab)
    values = qkv_proj[..., 2 * HEAD:]
    scores = jnp.einsum("qhd,khd->hqk", query.astype(jnp.float32), key_rot.astype(jnp.float32)) * HEAD ** -0.5
    causal = jnp.arange(SEQ)[:, None] >= jnp.arange(SEQ)[None, :]
    scores = jnp.where(causal[None], scores, -1e30)
    probs = jax.nn.softmax(scores, axis=-1).astype(jnp.bfloat16)
    context = jnp.einsum("hqk,khd->qhd", probs.astype(jnp.float32), values.astype(jnp.float32)).astype(jnp.bfloat16)
    attn_part = jnp.dot(context.reshape(SEQ, D), layer["w_dense"].reshape(D, D), preferred_element_type=jnp.float32)
    ln_mlp = layer_norm(x_row, layer["ln2_gain"], layer["ln2_bias"])
    hidden = jnp.dot(ln_mlp, layer["w_up"], preferred_element_type=jnp.float32) + layer["b_up"].astype(jnp.float32)
    hidden = jax.nn.gelu(hidden, approximate=False).astype(jnp.bfloat16)
    mlp_part = jnp.dot(hidden, layer["w_down"], preferred_element_type=jnp.float32)
    bias_sum = layer["b_dense"].astype(jnp.float32) + layer["b_down"].astype(jnp.float32)
    return (x_row.astype(jnp.float32) + bias_sum + attn_part + mlp_part).astype(jnp.bfloat16)


def reference(x_micro, ln1_gain, ln1_bias, w_qkv, b_qkv, w_dense, b_dense, ln2_gain, ln2_bias, w_up, b_up, w_down, b_down):
    cos_tab, sin_tab = rotary_tables()
    stacked = {
        "ln1_gain": ln1_gain, "ln1_bias": ln1_bias, "w_qkv": w_qkv, "b_qkv": b_qkv,
        "w_dense": w_dense, "b_dense": b_dense, "ln2_gain": ln2_gain, "ln2_bias": ln2_bias,
        "w_up": w_up, "b_up": b_up, "w_down": w_down, "b_down": b_down,
    }
    rows = x_micro.reshape(MICRO * BATCH, SEQ, D)

    def one_layer(carry, layer):
        return lax.map(lambda x_row: neox_row(x_row, layer, cos_tab, sin_tab), carry), None

    final, _ = lax.scan(one_layer, rows, stacked)
    return final.reshape(MICRO, BATCH, SEQ, D)
```

```python
import functools

import jax
import jax.numpy as jnp
import numpy as np
from jax import lax
from jax.experimental import pallas as pl
from jax.experimental.pallas import tpu as pltpu
from jax.sharding import PartitionSpec as P

MESH = pl.DeviceIdType.MESH
F32, BF16 = jnp.float32, jnp.bfloat16
X_SLOTS = 3
CHUNKS = 4
EAGER = 0


def rotary_lanes(seq_len, head_dim):
    rot = head_dim // 4
    half = rot // 2
    inv_freq = (1.0 / (np.float32(10000.0) ** (np.arange(0, rot, 2).astype(np.float32) / np.float32(rot)))).astype(np.float32)
    angles = np.arange(seq_len).astype(np.float32)[:, None] * inv_freq[None, :]
    cos, sin = np.cos(angles.astype(np.float64)), np.sin(angles.astype(np.float64))
    cos_l = np.ones((seq_len, head_dim), np.float32)
    sin_lo = np.zeros((seq_len, head_dim), np.float32)
    sin_hi = np.zeros((seq_len, head_dim), np.float32)
    cos_l[:, :half], cos_l[:, half:rot] = cos, cos
    sin_lo[:, :half] = -sin
    sin_hi[:, half:rot] = sin
    return cos_l, sin_lo, sin_hi


def kernel(dims, x_hbm, cos_ref, slo_ref, shi_ref, g1_ref, b1_ref, g2_ref, b2_ref, bqkv_ref, bup_ref, bd_ref, bdn_ref,
           wqkv_hbm, wd_hbm, wup_hbm, wdn_hbm, y_hbm,
           wqkv, wd, wup, wdn, xin, psend, precv, osend, a_ref, c_ref, qkv, ctx, hid, g1, b1, g2, b2, bqkv, bup, bias,
           w_sem, x_ls, x_rs, x_free, p_ss, p_rs, f_ss, b_ss, r_ss, y_rs):
    n_micro, n_st, seq, d, heads, hd, ffn = dims
    S, C = X_SLOTS, CHUNKS
    cw = d // C
    tp, st = lax.axis_index("tp"), lax.axis_index("pp")
    is_first, is_last = st == 0, st == n_st - 1
    not_first, not_last = st > 0, st < n_st - 1
    partner = (1 - tp, st)

    def cols(c):
        return pl.ds(c * cw, cw)

    w_copies = [pltpu.make_async_copy(src, dst, w_sem.at[k])
                for k, (src, dst) in enumerate(((wqkv_hbm, wqkv), (wup_hbm, wup), (wd_hbm, wd), (wdn_hbm, wdn)))]

    def x_load(m):
        s = lax.rem(m, S)
        return pltpu.make_async_copy(x_hbm.at[m], xin.at[s], x_ls.at[s])

    @pl.when(is_first)
    def _():
        for m in range(S):
            x_load(m).start()

    for cp in w_copies:
        cp.start()

    def p_copy(m, c):
        s = lax.rem(m, 2)
        return pltpu.make_async_remote_copy(psend.at[s, :, cols(c)], precv.at[s, :, cols(c)], p_ss.at[s, c], p_rs.at[s, c],
                                            device_id=partner, device_id_type=MESH)

    def f_copy(m, c):
        s, xs = lax.rem(m, 2), lax.rem(m, S)
        return pltpu.make_async_remote_copy(osend.at[s, :, cols(c)], xin.at[xs, :, cols(c)], f_ss.at[s, c], x_rs.at[xs, c],
                                            device_id=(tp, st + 1), device_id_type=MESH)

    def b_copies(m):
        s = lax.rem(m, 2)
        far = [pltpu.make_async_remote_copy(osend.at[s], y_hbm.at[m], b_ss.at[s, k], y_rs.at[m],
                                            device_id=(tp, target), device_id_type=MESH)
               for k, target in enumerate((n_st - 3, n_st - 5, n_st - 2))]
        return far + [pltpu.make_async_copy(osend.at[s], y_hbm.at[m], b_ss.at[s, 3])]

    def y_wait(m):
        pltpu.make_async_remote_copy(y_hbm.at[m], y_hbm.at[m], r_ss.at[0], y_rs.at[m],
                                     device_id=partner, device_id_type=MESH).wait_recv()

    def relay_copy(m, k, target):
        return pltpu.make_async_remote_copy(y_hbm.at[m], y_hbm.at[m], r_ss.at[k], y_rs.at[m],
                                            device_id=(tp, target), device_id_type=MESH)

    two_hop = st == n_st - 3
    relays = jnp.logical_and(lax.rem(st, 2) == 1, not_last)

    def relay(m):
        y_wait(m)

        @pl.when(m > 0)
        def _():
            relay_copy(m - 1, 0, st - 1).wait_send()

        relay_copy(m, 0, st - 1).start()

        @pl.when(two_hop)
        def _():
            @pl.when(m > 0)
            def _():
                relay_copy(m - 1, 1, 1).wait_send()

            relay_copy(m, 1, 1).start()

    delay = 3 + ((n_st - 1 - st) * 3) // 2

    for src, dst in ((g1_ref, g1), (b1_ref, b1), (g2_ref, g2), (b2_ref, b2), (bqkv_ref, bqkv), (bup_ref, bup)):
        dst[...] = src[...].astype(F32)
    bias[...] = bd_ref[...].astype(F32) + bdn_ref[...].astype(F32)

    def finish_chunk(m, c):
        s, xs = lax.rem(m, 2), lax.rem(m, S)
        p_copy(m, c).wait()

        @pl.when(m >= 2)
        def _():
            @pl.when(not_last)
            def _():
                f_copy(m - 2, c).wait_send()

            if c == 0:
                @pl.when(is_last)
                def _():
                    far = b_copies(m - 2)
                    for cp in far[:-1]:
                        cp.wait_send()
                    far[-1].wait()

        both = psend[s, :, cols(c)].astype(F32) + precv[s, :, cols(c)].astype(F32)
        base = xin[xs, :, cols(c)].astype(F32) + bias[:, cols(c)]
        osend[s, :, cols(c)] = (base + both).astype(BF16)

        @pl.when(not_last)
        def _():
            if c == 0:
                @pl.when(m >= S)
                def _():
                    pl.semaphore_wait(x_free, 1)
            f_copy(m, c).start()

        if c == C - 1:
            @pl.when(is_last)
            def _():
                for cp in b_copies(m):
                    cp.start()

            @pl.when(m + S < n_micro)
            def _():
                @pl.when(not_first)
                def _():
                    pl.semaphore_signal(x_free, inc=1, device_id=(tp, st - 1), device_id_type=MESH)

                @pl.when(is_first)
                def _():
                    x_load(m + S).start()

    def front(i):
        xs = lax.rem(i, S)
        rows_per = 16
        for r in range(seq // rows_per):
            rows = pl.ds(r * rows_per, rows_per)
            x_f32 = xin[xs, rows, :].astype(F32)
            centered = x_f32 - jnp.mean(x_f32, axis=-1, keepdims=True)
            spread = jnp.mean(centered * centered, axis=-1, keepdims=True)
            normed = centered * lax.rsqrt(spread + 1e-5)
            a_ref[rows, :] = (normed * g1[...] + b1[...]).astype(BF16)
            c_ref[rows, :] = (normed * g2[...] + b2[...]).astype(BF16)

        a = a_ref[...]
        qw = 2 * 3 * hd
        lane = lax.broadcasted_iota(jnp.int32, (seq, hd), 1)
        rot = hd // 4
        for q in range(heads * 3 * hd // qw):
            cs = pl.ds(q * qw, qw)
            part = jnp.dot(a, wqkv[:, cs], preferred_element_type=F32)
            qkv[:, cs] = (part + bqkv[:, cs]).astype(BF16)

        def rotate(v):
            v = v.astype(F32)
            mixed = v * cos_ref[...] + (pltpu.roll(v, hd - rot // 2, 1) * slo_ref[...] + pltpu.roll(v, rot // 2, 1) * shi_ref[...])
            return jnp.where(lane < rot, mixed, v).astype(BF16)

        causal = lax.broadcasted_iota(jnp.int32, (seq, seq), 0) >= lax.broadcasted_iota(jnp.int32, (seq, seq), 1)
        for h in range(heads):
            base = h * 3 * hd
            query = rotate(qkv[:, pl.ds(base, hd)])
            key = rotate(qkv[:, pl.ds(base + hd, hd)])
            value = qkv[:, pl.ds(base + 2 * hd, hd)]
            scores = lax.dot_general(query, key, (((1,), (1,)), ((), ())), preferred_element_type=F32) * hd ** -0.5
            scores = jnp.where(causal, scores, -1e30)
            top = jnp.max(scores, axis=-1, keepdims=True)
            e = jnp.exp(scores - top)
            probs = (e / jnp.sum(e, axis=-1, keepdims=True)).astype(BF16)
            ctx[:, pl.ds(h * hd, hd)] = jnp.dot(probs, value, preferred_element_type=F32).astype(BF16)

        c = c_ref[...]
        uw = 512
        for u in range(ffn // uw):
            cs = pl.ds(u * uw, uw)
            up = jnp.dot(c, wup[:, cs], preferred_element_type=F32) + bup[:, cs]
            gelu = 0.5 * up * (1.0 + lax.erf(up * np.float32(np.sqrt(0.5))))
            hid[:, cs] = gelu.astype(BF16)

    def back_chunk(i, c):
        part = jnp.dot(hid[...], wdn[:, cols(c)], preferred_element_type=F32)
        part = part + jnp.dot(ctx[...], wd[:, cols(c)], preferred_element_type=F32)
        psend[lax.rem(i, 2), :, cols(c)] = part.astype(BF16)
        p_copy(i, c).start()

    w_copies[0].wait()
    w_copies[1].wait()

    def body(i, carry):
        @pl.when(is_first)
        def _():
            x_load(i).wait()

        @pl.when(not_first)
        def _():
            for c in range(C):
                f_copy(i, c).wait_recv()

        front(i)

        @pl.when(i == 0)
        def _():
            w_copies[2].wait()
            w_copies[3].wait()

        for c in range(C):
            @pl.when(i - 1 >= EAGER)
            def _():
                finish_chunk(i - 1, c)

            back_chunk(i, c)

        @pl.when(i < EAGER)
        def _():
            for c in range(C):
                finish_chunk(i, c)

        @pl.when(jnp.logical_and(relays, i >= delay))
        def _():
            relay(i - delay)

        return carry

    lax.fori_loop(0, n_micro, body, 0)
    last = n_micro - 1
    for c in range(C):
        finish_chunk(last, c)

    @pl.when(not_last)
    def _():
        for m in (n_micro - 2, n_micro - 1):
            for c in range(C):
                f_copy(m, c).wait_send()

    @pl.when(is_last)
    def _():
        for m in (n_micro - 2, n_micro - 1):
            far = b_copies(m)
            for cp in far[:-1]:
                cp.wait_send()
            far[-1].wait()

    @pl.when(relays)
    def _():
        def more(m, carry):
            relay(m)
            return carry

        lax.fori_loop(jnp.maximum(n_micro - delay, 0), n_micro, more, 0)
        relay_copy(last, 0, st - 1).wait_send()

        @pl.when(two_hop)
        def _():
            relay_copy(last, 1, 1).wait_send()

    @pl.when(lax.rem(st, 2) == 0)
    def _():
        def leaf(m, carry):
            y_wait(m)
            return carry

        lax.fori_loop(0, n_micro, leaf, 0)


def solution(mesh):
    n_st = mesh.shape["pp"]
    in_specs = (P(), P("pp", None), P("pp", None), P("pp", None, "tp", None), P("pp", "tp", None),
                P("pp", "tp", None, None), P("pp", None), P("pp", None), P("pp", None),
                P("pp", None, "tp"), P("pp", "tp"), P("pp", "tp", None), P("pp", None))

    def device_fn(x_micro, ln1_gain, ln1_bias, w_qkv, b_qkv, w_dense, b_dense, ln2_gain, ln2_bias, w_up, b_up, w_down, b_down):
        n_micro, _, seq, d = x_micro.shape
        heads, hd = w_dense.shape[1], w_dense.shape[2]
        ffn = w_up.shape[2]
        cos_l, sin_lo, sin_hi = rotary_lanes(seq, hd)
        dims = (n_micro, n_st, seq, d, heads, hd, ffn)
        vm = pl.BlockSpec(memory_space=pltpu.VMEM)
        hbm = pl.BlockSpec(memory_space=pl.ANY)
        dma = pltpu.SemaphoreType.DMA
        S, C = X_SLOTS, CHUNKS
        out = pl.pallas_call(
            functools.partial(kernel, dims),
            out_shape=jax.ShapeDtypeStruct((n_micro, seq, d), BF16),
            in_specs=[hbm] + [vm] * 11 + [hbm] * 4,
            out_specs=hbm,
            scratch_shapes=[
                pltpu.VMEM((d, heads * 3 * hd), BF16), pltpu.VMEM((heads * hd, d), BF16),
                pltpu.VMEM((d, ffn), BF16), pltpu.VMEM((ffn, d), BF16),
                pltpu.VMEM((S, seq, d), BF16), pltpu.VMEM((2, seq, d), BF16), pltpu.VMEM((2, seq, d), BF16),
                pltpu.VMEM((2, seq, d), BF16),
                pltpu.VMEM((seq, d), BF16), pltpu.VMEM((seq, d), BF16),
                pltpu.VMEM((seq, heads * 3 * hd), BF16), pltpu.VMEM((seq, heads * hd), BF16), pltpu.VMEM((seq, ffn), BF16),
                pltpu.VMEM((1, d), F32), pltpu.VMEM((1, d), F32), pltpu.VMEM((1, d), F32), pltpu.VMEM((1, d), F32),
                pltpu.VMEM((1, heads * 3 * hd), F32), pltpu.VMEM((1, ffn), F32), pltpu.VMEM((1, d), F32),
                dma((4,)), dma((S,)), dma((S, C)), pltpu.SemaphoreType.REGULAR,
                dma((2, C)), dma((2, C)), dma((2, C)), dma((2, 4)), dma((2,)), dma((n_micro,)),
            ],
            compiler_params=pltpu.CompilerParams(has_side_effects=True, vmem_limit_bytes=67_043_328),
            name="neox_pipeline",
        )(x_micro.reshape(n_micro, seq, d), jnp.asarray(cos_l), jnp.asarray(sin_lo), jnp.asarray(sin_hi),
          ln1_gain, ln1_bias, ln2_gain, ln2_bias, b_qkv.reshape(1, -1), b_up, b_dense, b_down,
          w_qkv.reshape(d, heads * 3 * hd), w_dense.reshape(heads * hd, d), w_up[0], w_down[0])
        return out.reshape(x_micro.shape)

    return jax.shard_map(device_fn, mesh=mesh, in_specs=in_specs, out_specs=P(), check_vma=False)
```

```python
import functools

import jax
import jax.numpy as jnp
import numpy as np
from jax import lax
from jax.experimental import pallas as pl
from jax.experimental.pallas import tpu as pltpu
from jax.sharding import PartitionSpec as P

MESH = pl.DeviceIdType.MESH
F32, BF16 = jnp.float32, jnp.bfloat16
X_SLOTS = 4
CHUNKS = 4
SUM_AT = (1, 1, 3, 3)
K_BLOCK = 128


def rotary_lanes(seq_len, head_dim):
    rot = head_dim // 4
    half = rot // 2
    inv_freq = (1.0 / (np.float32(10000.0) ** (np.arange(0, rot, 2).astype(np.float32) / np.float32(rot)))).astype(np.float32)
    angles = np.arange(seq_len).astype(np.float32)[:, None] * inv_freq[None, :]
    cos, sin = np.cos(angles.astype(np.float64)), np.sin(angles.astype(np.float64))
    cos_l = np.ones((seq_len, head_dim), np.float32)
    sin_lo = np.zeros((seq_len, head_dim), np.float32)
    sin_hi = np.zeros((seq_len, head_dim), np.float32)
    cos_l[:, :half], cos_l[:, half:rot] = cos, cos
    sin_lo[:, :half] = -sin
    sin_hi[:, half:rot] = sin
    return cos_l, sin_lo, sin_hi


def kernel(dims, x_hbm, cos_ref, slo_ref, shi_ref, g1_ref, b1_ref, g2_ref, b2_ref, bqkv_ref, bup_ref, bd_ref, bdn_ref,
           wqkv_hbm, wd_hbm, wup_hbm, wdn_hbm, y_hbm,
           wq_in, wq_f32, wqkv, wd, wup, wdn, xin, psend, precv, osend, a_ref, c_ref, qkv, probs, ctx, hid, g1, b1, g2, b2, bqkv, bup, bias,
           w_sem, wq_sem, x_ls, x_rs, x_free, p_ss, p_rs, f_ss, b_ss, r_ss, y_rs):
    n_micro, n_st, seq, d, heads, hd, ffn = dims
    S, C = X_SLOTS, CHUNKS
    cw = d // C
    tp, st = lax.axis_index("tp"), lax.axis_index("pp")
    is_first, is_last = st == 0, st == n_st - 1
    not_first, not_last = st > 0, st < n_st - 1
    partner = (1 - tp, st)

    def cols(c):
        return pl.ds(c * cw, cw)

    def w_copy(k):
        src, dst = ((wup_hbm, wup), (wd_hbm, wd), (wdn_hbm, wdn))[k]
        return pltpu.make_async_copy(src, dst, w_sem.at[k])

    def wq_load(kb):
        return pltpu.make_async_copy(wqkv_hbm.at[pl.ds(kb * K_BLOCK, K_BLOCK)], wq_in.at[lax.rem(kb, 2)], wq_sem.at[lax.rem(kb, 2)])

    def x_load(m):
        s = lax.rem(m, S)
        return pltpu.make_async_copy(x_hbm.at[m], xin.at[s], x_ls.at[s])

    @pl.when(is_first)
    def _():
        for m in range(S):
            x_load(m).start()

    wq_load(0).start()
    wq_load(1).start()

    def p_copy(m, c):
        s = lax.rem(m, 2)
        return pltpu.make_async_remote_copy(psend.at[s, :, cols(c)], precv.at[s, :, cols(c)], p_ss.at[s, c], p_rs.at[s, c],
                                            device_id=partner, device_id_type=MESH)

    def f_copy(m, c):
        s, xs = lax.rem(m, 2), lax.rem(m, S)
        return pltpu.make_async_remote_copy(osend.at[s, :, cols(c)], xin.at[xs, :, cols(c)], f_ss.at[s, c], x_rs.at[xs, c],
                                            device_id=(tp, st + 1), device_id_type=MESH)

    def b_copies(m, c):
        s = lax.rem(m, 2)
        src, dst = osend.at[s, :, cols(c)], y_hbm.at[m, :, cols(c)]
        far = [pltpu.make_async_remote_copy(src, dst, b_ss.at[s, k, c], y_rs.at[m, c], device_id=(tp, target), device_id_type=MESH)
               for k, target in enumerate((n_st - 3, n_st - 5, n_st - 2))]
        return far + [pltpu.make_async_copy(src, dst, b_ss.at[s, 3, c])]

    def b_wait(m, c):
        copies = b_copies(m, c)
        for cp in copies[:-1]:
            cp.wait_send()
        copies[-1].wait()

    def relay_copy(m, c, k, target):
        here = y_hbm.at[m, :, cols(c)]
        return pltpu.make_async_remote_copy(here, here, r_ss.at[k, c], y_rs.at[m, c], device_id=(tp, target), device_id_type=MESH)

    def y_wait(m, c):
        relay_copy(m, c, 0, 0).wait_recv()

    two_hop = st == n_st - 3
    relays = jnp.logical_and(lax.rem(st, 2) == 1, not_last)

    def relay(m):
        for c in range(C):
            y_wait(m, c)

            @pl.when(m > 0)
            def _():
                relay_copy(m - 1, c, 0, st - 1).wait_send()

            relay_copy(m, c, 0, st - 1).start()

            @pl.when(two_hop)
            def _():
                @pl.when(m > 0)
                def _():
                    relay_copy(m - 1, c, 1, 1).wait_send()

                relay_copy(m, c, 1, 1).start()

    ahead = n_st - 1 - st
    delay = 4 + ahead + (ahead * ahead + 2) // 3

    for src, dst in ((g1_ref, g1), (b1_ref, b1), (g2_ref, g2), (b2_ref, b2), (bup_ref, bup)):
        dst[...] = src[...].astype(F32)
    for h in range(heads):
        bqkv[:, pl.ds(h * 3 * hd, 3 * hd)] = bqkv_ref[pl.ds(h, 1), :].astype(F32)
    bias[...] = bd_ref[...].astype(F32) + bdn_ref[...].astype(F32)

    n_kb = d // K_BLOCK
    up_rows = d // n_kb

    def lay_out(kb, carry):
        rows = pl.ds(pl.multiple_of(kb * K_BLOCK, K_BLOCK), K_BLOCK)
        up_r = pl.ds(kb * up_rows, up_rows)
        pltpu.make_async_copy(wup_hbm.at[up_r], wup.at[up_r], w_sem.at[0]).start()
        wq_load(kb).wait()
        for e in range(3 * hd // 128):
            wq_f32[e] = wq_in[lax.rem(kb, 2), :, :, pl.ds(e * 128, 128)].astype(F32).reshape(K_BLOCK * heads, 128)

        @pl.when(kb + 2 < n_kb)
        def _():
            wq_load(kb + 2).start()

        for h in range(heads):
            for e in range(3 * hd // 128):
                wqkv[rows, pl.ds(h * 3 * hd + e * 128, 128)] = wq_f32[e, pl.ds(h, K_BLOCK, stride=heads), :].astype(BF16)
        return carry

    def finish_chunk(m, c):
        s, xs = lax.rem(m, 2), lax.rem(m, S)
        p_copy(m, c).wait()

        @pl.when(m >= 2)
        def _():
            @pl.when(not_last)
            def _():
                f_copy(m - 2, c).wait_send()

            @pl.when(is_last)
            def _():
                b_wait(m - 2, c)

        both = psend[s, :, cols(c)].astype(F32) + precv[s, :, cols(c)].astype(F32)
        base = xin[xs, :, cols(c)].astype(F32) + bias[:, cols(c)]
        osend[s, :, cols(c)] = (base + both).astype(BF16)

        @pl.when(not_last)
        def _():
            if c == 0:
                @pl.when(m >= S)
                def _():
                    pl.semaphore_wait(x_free, 1)
            f_copy(m, c).start()

        @pl.when(is_last)
        def _():
            for cp in b_copies(m, c):
                cp.start()

        if c == C - 1:
            @pl.when(m + S < n_micro)
            def _():
                @pl.when(not_first)
                def _():
                    pl.semaphore_signal(x_free, inc=1, device_id=(tp, st - 1), device_id_type=MESH)

                @pl.when(is_first)
                def _():
                    x_load(m + S).start()

    def attention_part(i):
        xs = lax.rem(i, S)
        rows_per = 16
        for r in range(seq // rows_per):
            rows = pl.ds(r * rows_per, rows_per)
            x_f32 = xin[xs, rows, :].astype(F32)
            centered = x_f32 - jnp.mean(x_f32, axis=-1, keepdims=True)
            spread = jnp.mean(centered * centered, axis=-1, keepdims=True)
            normed = centered * lax.rsqrt(spread + 1e-5)
            a_ref[rows, :] = (normed * g1[...] + b1[...]).astype(BF16)
            c_ref[rows, :] = (normed * g2[...] + b2[...]).astype(BF16)

        a = a_ref[...]
        qw = 2 * 3 * hd
        lane = lax.broadcasted_iota(jnp.int32, (seq, hd), 1)
        rot = hd // 4
        def rotate(v):
            v = v.astype(F32)
            mixed = v * cos_ref[...] + (pltpu.roll(v, hd - rot // 2, 1) * slo_ref[...] + pltpu.roll(v, rot // 2, 1) * shi_ref[...])
            return jnp.where(lane < rot, mixed, v).astype(BF16)

        causal = lax.broadcasted_iota(jnp.int32, (seq, seq), 0) >= lax.broadcasted_iota(jnp.int32, (seq, seq), 1)
        def head_probs(h):
            base = h * 3 * hd
            query = rotate(qkv[:, pl.ds(base, hd)])
            key = rotate(qkv[:, pl.ds(base + hd, hd)])
            scores = lax.dot_general(query, key, (((1,), (1,)), ((), ())), preferred_element_type=F32) * hd ** -0.5
            scores = jnp.where(causal, scores, -1e30)
            top = jnp.max(scores, axis=-1, keepdims=True)
            e = jnp.exp(scores - top)
            probs[h] = (e / jnp.sum(e, axis=-1, keepdims=True)).astype(BF16)

        n_q = heads * 3 * hd // qw
        for q in range(n_q + 1):
            if q < n_q:
                cs = pl.ds(q * qw, qw)
                part = jnp.dot(a, wqkv[:, cs], preferred_element_type=F32)
                qkv[:, cs] = (part + bqkv[:, cs]).astype(BF16)
            if q > 0:
                for h in range(2 * (q - 1), 2 * q):
                    head_probs(h)

    def up_part(part):
        c = c_ref[...]
        uw = 512
        half = ffn // uw // 2
        for u in range(part * half, (part + 1) * half):
            cs = pl.ds(u * uw, uw)
            up = jnp.dot(c, wup[:, cs], preferred_element_type=F32) + bup[:, cs]
            gelu = 0.5 * up * (1.0 + lax.erf(up * np.float32(np.sqrt(0.5))))
            hid[:, cs] = gelu.astype(BF16)
            n_u = ffn // uw
            for h in range(heads):
                if u == min(1 + h * n_u // heads, n_u - 1):
                    value = qkv[:, pl.ds(h * 3 * hd + 2 * hd, hd)]
                    ctx[:, pl.ds(h * hd, hd)] = jnp.dot(probs[h], value, preferred_element_type=F32).astype(BF16)

    def back_chunk(i, c):
        part = jnp.dot(hid[...], wdn[:, cols(c)], preferred_element_type=F32)
        part = part + jnp.dot(ctx[...], wd[:, cols(c)], preferred_element_type=F32)
        psend[lax.rem(i, 2), :, cols(c)] = part.astype(BF16)
        p_copy(i, c).start()

    lax.fori_loop(0, n_kb, lay_out, 0)
    w_copy(1).start()
    w_copy(2).start()

    def body(i, carry):
        def sums(where):
            here = [c for c in range(C) if SUM_AT[c] == where]
            if here:
                @pl.when(i > 0)
                def _():
                    for c in here:
                        finish_chunk(i - 1, c)

        sums(0)

        @pl.when(is_first)
        def _():
            x_load(i).wait()

        @pl.when(not_first)
        def _():
            for c in range(C):
                f_copy(i, c).wait_recv()

        attention_part(i)

        @pl.when(i == 0)
        def _():
            w_copy(0).wait()

        sums(1)
        up_part(0)
        sums(2)
        up_part(1)

        @pl.when(i == 0)
        def _():
            w_copy(1).wait()
            w_copy(2).wait()

        sums(3)
        for c in range(C):
            back_chunk(i, c)
            sums(4 + c)

        @pl.when(jnp.logical_and(relays, i >= delay))
        def _():
            relay(i - delay)

        return carry

    lax.fori_loop(0, n_micro, body, 0)
    last = n_micro - 1
    for c in range(C):
        finish_chunk(last, c)

    @pl.when(not_last)
    def _():
        for m in (n_micro - 2, n_micro - 1):
            for c in range(C):
                f_copy(m, c).wait_send()

    @pl.when(is_last)
    def _():
        for m in (n_micro - 2, n_micro - 1):
            for c in range(C):
                b_wait(m, c)

    @pl.when(relays)
    def _():
        def more(m, carry):
            relay(m)
            return carry

        lax.fori_loop(jnp.maximum(n_micro - delay, 0), n_micro, more, 0)
        for c in range(C):
            relay_copy(last, c, 0, st - 1).wait_send()

        @pl.when(two_hop)
        def _():
            for c in range(C):
                relay_copy(last, c, 1, 1).wait_send()

    @pl.when(lax.rem(st, 2) == 0)
    def _():
        def leaf(m, carry):
            for c in range(C):
                y_wait(m, c)
            return carry

        lax.fori_loop(0, n_micro, leaf, 0)


def copy_kernel(n, src_hbm, dst_hbm, buf, in_sem, out_sem):
    loads = [pltpu.make_async_copy(src_hbm.at[m], buf.at[m], in_sem.at[m]) for m in range(n)]
    stores = [pltpu.make_async_copy(buf.at[m], dst_hbm.at[m], out_sem.at[m]) for m in range(n)]
    for cp in loads:
        cp.start()
    for load, store in zip(loads, stores):
        load.wait()
        store.start()
    for cp in stores:
        cp.wait()


def solution(mesh):
    n_st = mesh.shape["pp"]
    in_specs = (P(), P("pp", None), P("pp", None), P("pp", None, "tp", None), P("pp", "tp", None),
                P("pp", "tp", None, None), P("pp", None), P("pp", None), P("pp", None),
                P("pp", None, "tp"), P("pp", "tp"), P("pp", "tp", None), P("pp", None))

    def device_fn(x_micro, ln1_gain, ln1_bias, w_qkv, b_qkv, w_dense, b_dense, ln2_gain, ln2_bias, w_up, b_up, w_down, b_down):
        n_micro, _, seq, d = x_micro.shape
        heads, hd = w_dense.shape[1], w_dense.shape[2]
        ffn = w_up.shape[2]
        cos_l, sin_lo, sin_hi = rotary_lanes(seq, hd)
        dims = (n_micro, n_st, seq, d, heads, hd, ffn)
        vm = pl.BlockSpec(memory_space=pltpu.VMEM)
        hbm = pl.BlockSpec(memory_space=pl.ANY)
        dma = pltpu.SemaphoreType.DMA
        S, C = X_SLOTS, CHUNKS
        out = pl.pallas_call(
            functools.partial(kernel, dims),
            out_shape=jax.ShapeDtypeStruct((n_micro, seq, d), BF16),
            in_specs=[hbm] + [vm] * 11 + [hbm] * 4,
            out_specs=hbm,
            scratch_shapes=[
                pltpu.VMEM((2, K_BLOCK, heads, 3 * hd), BF16), pltpu.VMEM((3 * hd // 128, K_BLOCK * heads, 128), F32),
                pltpu.VMEM((d, heads * 3 * hd), BF16), pltpu.VMEM((heads * hd, d), BF16),
                pltpu.VMEM((d, ffn), BF16), pltpu.VMEM((ffn, d), BF16),
                pltpu.VMEM((S, seq, d), BF16), pltpu.VMEM((2, seq, d), BF16), pltpu.VMEM((2, seq, d), BF16),
                pltpu.VMEM((2, seq, d), BF16),
                pltpu.VMEM((seq, d), BF16), pltpu.VMEM((seq, d), BF16),
                pltpu.VMEM((seq, heads * 3 * hd), BF16), pltpu.VMEM((heads, seq, seq), BF16), pltpu.VMEM((seq, heads * hd), BF16), pltpu.VMEM((seq, ffn), BF16),
                pltpu.VMEM((1, d), F32), pltpu.VMEM((1, d), F32), pltpu.VMEM((1, d), F32), pltpu.VMEM((1, d), F32),
                pltpu.VMEM((1, heads * 3 * hd), F32), pltpu.VMEM((1, ffn), F32), pltpu.VMEM((1, d), F32),
                dma((3,)), dma((2,)), dma((S,)), dma((S, C)), pltpu.SemaphoreType.REGULAR,
                dma((2, C)), dma((2, C)), dma((2, C)), dma((2, 4, C)), dma((2, C)), dma((n_micro, C)),
            ],
            compiler_params=pltpu.CompilerParams(has_side_effects=True, vmem_limit_bytes=67_043_328),
            name="neox_pipeline",
        )(x_micro.reshape(n_micro, seq, d), jnp.asarray(cos_l), jnp.asarray(sin_lo), jnp.asarray(sin_hi),
          ln1_gain, ln1_bias, ln2_gain, ln2_bias, b_qkv[0], b_up, b_dense, b_down,
          w_qkv[0], w_dense.reshape(heads * hd, d), w_up[0], w_down[0])
        out = pl.pallas_call(functools.partial(copy_kernel, n_micro), out_shape=jax.ShapeDtypeStruct(out.shape, BF16),
                             in_specs=[hbm], out_specs=hbm,
                             scratch_shapes=[pltpu.VMEM(out.shape, BF16), dma((n_micro,)), dma((n_micro,))],
                             compiler_params=pltpu.CompilerParams(vmem_limit_bytes=40_000_000), name="result_copy")(out)
        return out.reshape(x_micro.shape)

    return jax.shard_map(device_fn, mesh=mesh, in_specs=in_specs, out_specs=P(), check_vma=False)
```

```python
import functools

import jax
import jax.numpy as jnp
import numpy as np
from jax import lax
from jax.experimental import pallas as pl
from jax.experimental.pallas import tpu as pltpu
from jax.sharding import PartitionSpec as P

MESH = pl.DeviceIdType.MESH
F32, BF16 = jnp.float32, jnp.bfloat16
X_SLOTS = 4
CHUNKS = 4
SUM_AT = (1, 1, 3, 3)
K_BLOCK = 128


def rotary_lanes(seq_len, head_dim):
    rot = head_dim // 4
    half = rot // 2
    inv_freq = (1.0 / (np.float32(10000.0) ** (np.arange(0, rot, 2).astype(np.float32) / np.float32(rot)))).astype(np.float32)
    angles = np.arange(seq_len).astype(np.float32)[:, None] * inv_freq[None, :]
    cos, sin = np.cos(angles.astype(np.float64)), np.sin(angles.astype(np.float64))
    cos_l = np.ones((seq_len, head_dim), np.float32)
    sin_lo = np.zeros((seq_len, head_dim), np.float32)
    sin_hi = np.zeros((seq_len, head_dim), np.float32)
    cos_l[:, :half], cos_l[:, half:rot] = cos, cos
    sin_lo[:, :half] = -sin
    sin_hi[:, half:rot] = sin
    return cos_l, sin_lo, sin_hi


def kernel(dims, x_hbm, cos_ref, slo_ref, shi_ref, g1_ref, b1_ref, g2_ref, b2_ref, bqkv_ref, bup_ref, bd_ref, bdn_ref,
           wqkv_hbm, wd_hbm, wup_hbm, wdn_hbm, y_hbm,
           wq_in, wq_f32, wqkv, wd, wup, wdn, xin, psend, precv, osend, a_ref, c_ref, qkv, probs, ctx, hid, g1, b1, g2, b2, bqkv, bup, bias,
           w_sem, wq_sem, x_ls, x_rs, x_free, p_ss, p_rs, f_ss, b_ss, r_ss, y_rs):
    n_micro, n_st, seq, d, heads, hd, ffn = dims
    S, C = X_SLOTS, CHUNKS
    cw = d // C
    tp, st = lax.axis_index("tp"), lax.axis_index("pp")
    is_first, is_last = st == 0, st == n_st - 1
    not_first, not_last = st > 0, st < n_st - 1
    partner = (1 - tp, st)

    def cols(c):
        return pl.ds(c * cw, cw)

    def w_copy(k):
        src, dst = ((wup_hbm, wup), (wd_hbm, wd), (wdn_hbm, wdn))[k]
        return pltpu.make_async_copy(src, dst, w_sem.at[k])

    def wq_load(kb):
        return pltpu.make_async_copy(wqkv_hbm.at[pl.ds(kb * K_BLOCK, K_BLOCK)], wq_in.at[lax.rem(kb, 2)], wq_sem.at[lax.rem(kb, 2)])

    def x_load(m):
        s = lax.rem(m, S)
        return pltpu.make_async_copy(x_hbm.at[m], xin.at[s], x_ls.at[s])

    @pl.when(is_first)
    def _():
        for m in range(S):
            x_load(m).start()

    wq_load(0).start()
    wq_load(1).start()

    def p_copy(m, c):
        s = lax.rem(m, 2)
        return pltpu.make_async_remote_copy(psend.at[s, :, cols(c)], precv.at[s, :, cols(c)], p_ss.at[s, c], p_rs.at[s, c],
                                            device_id=partner, device_id_type=MESH)

    def f_copy(m, c):
        s, xs = lax.rem(m, 2), lax.rem(m, S)
        return pltpu.make_async_remote_copy(osend.at[s, :, cols(c)], xin.at[xs, :, cols(c)], f_ss.at[s, c], x_rs.at[xs, c],
                                            device_id=(tp, st + 1), device_id_type=MESH)

    def b_copies(m, c):
        s = lax.rem(m, 2)
        src, dst = osend.at[s, :, cols(c)], y_hbm.at[m, :, cols(c)]
        far = [pltpu.make_async_remote_copy(src, dst, b_ss.at[s, k, c], y_rs.at[m, c], device_id=(tp, target), device_id_type=MESH)
               for k, target in enumerate((n_st - 3, n_st - 5, n_st - 2))]
        return far + [pltpu.make_async_copy(src, dst, b_ss.at[s, 3, c])]

    def b_wait(m, c):
        copies = b_copies(m, c)
        for cp in copies[:-1]:
            cp.wait_send()
        copies[-1].wait()

    def relay_copy(m, c, k, target):
        here = y_hbm.at[m, :, cols(c)]
        return pltpu.make_async_remote_copy(here, here, r_ss.at[k, c], y_rs.at[m, c], device_id=(tp, target), device_id_type=MESH)

    def y_wait(m, c):
        relay_copy(m, c, 0, 0).wait_recv()

    two_hop = st == n_st - 3
    relays = jnp.logical_and(lax.rem(st, 2) == 1, not_last)

    def relay(m):
        for c in range(C):
            y_wait(m, c)

            @pl.when(m > 0)
            def _():
                relay_copy(m - 1, c, 0, st - 1).wait_send()

            relay_copy(m, c, 0, st - 1).start()

            @pl.when(two_hop)
            def _():
                @pl.when(m > 0)
                def _():
                    relay_copy(m - 1, c, 1, 1).wait_send()

                relay_copy(m, c, 1, 1).start()

    ahead = n_st - 1 - st
    delay = 4 + ahead + (ahead * ahead + 2) // 3

    for src, dst in ((g1_ref, g1), (b1_ref, b1), (g2_ref, g2), (b2_ref, b2), (bup_ref, bup)):
        dst[...] = src[...].astype(F32)
    for h in range(heads):
        bqkv[:, pl.ds(h * 3 * hd, 3 * hd)] = bqkv_ref[pl.ds(h, 1), :].astype(F32)
    bias[...] = bd_ref[...].astype(F32) + bdn_ref[...].astype(F32)

    n_kb = d // K_BLOCK
    up_rows = d // n_kb

    def lay_out(kb, carry):
        rows = pl.ds(pl.multiple_of(kb * K_BLOCK, K_BLOCK), K_BLOCK)
        up_r = pl.ds(kb * up_rows, up_rows)
        pltpu.make_async_copy(wup_hbm.at[up_r], wup.at[up_r], w_sem.at[0]).start()
        wq_load(kb).wait()
        for e in range(3 * hd // 128):
            wq_f32[e] = wq_in[lax.rem(kb, 2), :, :, pl.ds(e * 128, 128)].astype(F32).reshape(K_BLOCK * heads, 128)

        @pl.when(kb + 2 < n_kb)
        def _():
            wq_load(kb + 2).start()

        for h in range(heads):
            for e in range(3 * hd // 128):
                wqkv[rows, pl.ds(h * 3 * hd + e * 128, 128)] = wq_f32[e, pl.ds(h, K_BLOCK, stride=heads), :].astype(BF16)
        return carry

    def finish_chunk(m, c):
        s, xs = lax.rem(m, 2), lax.rem(m, S)
        p_copy(m, c).wait()

        @pl.when(m >= 2)
        def _():
            @pl.when(not_last)
            def _():
                f_copy(m - 2, c).wait_send()

            @pl.when(is_last)
            def _():
                b_wait(m - 2, c)

        both = psend[s, :, cols(c)].astype(F32) + precv[s, :, cols(c)].astype(F32)
        base = xin[xs, :, cols(c)].astype(F32) + bias[:, cols(c)]
        osend[s, :, cols(c)] = (base + both).astype(BF16)

        @pl.when(not_last)
        def _():
            if c == 0:
                @pl.when(m >= S)
                def _():
                    pl.semaphore_wait(x_free, 1)
            f_copy(m, c).start()

        @pl.when(is_last)
        def _():
            for cp in b_copies(m, c):
                cp.start()

        if c == C - 1:
            @pl.when(m + S < n_micro)
            def _():
                @pl.when(not_first)
                def _():
                    pl.semaphore_signal(x_free, inc=1, device_id=(tp, st - 1), device_id_type=MESH)

                @pl.when(is_first)
                def _():
                    x_load(m + S).start()

    lane = lax.broadcasted_iota(jnp.int32, (seq, hd), 1)
    rot = hd // 4
    def rotate(v):
        v = v.astype(F32)
        mixed = v * cos_ref[...] + (pltpu.roll(v, hd - rot // 2, 1) * slo_ref[...] + pltpu.roll(v, rot // 2, 1) * shi_ref[...])
        return jnp.where(lane < rot, mixed, v).astype(BF16)

    causal = lax.broadcasted_iota(jnp.int32, (seq, seq), 0) >= lax.broadcasted_iota(jnp.int32, (seq, seq), 1)
    def head_probs(h):
        base = h * 3 * hd
        query = rotate(qkv[:, pl.ds(base, hd)])
        key = rotate(qkv[:, pl.ds(base + hd, hd)])
        scores = lax.dot_general(query, key, (((1,), (1,)), ((), ())), preferred_element_type=F32) * hd ** -0.5
        scores = jnp.where(causal, scores, -1e30)
        top = jnp.max(scores, axis=-1, keepdims=True)
        e = jnp.exp(scores - top)
        probs[h] = (e / jnp.sum(e, axis=-1, keepdims=True)).astype(BF16)

    def attention_part(i):
        xs = lax.rem(i, S)
        rows_per = 16
        for r in range(seq // rows_per):
            rows = pl.ds(r * rows_per, rows_per)
            x_f32 = xin[xs, rows, :].astype(F32)
            centered = x_f32 - jnp.mean(x_f32, axis=-1, keepdims=True)
            spread = jnp.mean(centered * centered, axis=-1, keepdims=True)
            normed = centered * lax.rsqrt(spread + 1e-5)
            a_ref[rows, :] = (normed * g1[...] + b1[...]).astype(BF16)
            c_ref[rows, :] = (normed * g2[...] + b2[...]).astype(BF16)

        a = a_ref[...]
        qw = 2 * 3 * hd
        n_q = heads * 3 * hd // qw
        for q in range(n_q):
            cs = pl.ds(q * qw, qw)
            part = jnp.dot(a, wqkv[:, cs], preferred_element_type=F32)
            qkv[:, cs] = (part + bqkv[:, cs]).astype(BF16)
            if q > 0:
                for h in range(2 * (q - 1), 2 * q):
                    head_probs(h)

    def up_part(part):
        c = c_ref[...]
        uw = 512
        half = ffn // uw // 2
        for u in range(part * half, (part + 1) * half):
            cs = pl.ds(u * uw, uw)
            up = jnp.dot(c, wup[:, cs], preferred_element_type=F32) + bup[:, cs]
            gelu = 0.5 * up * (1.0 + lax.erf(up * np.float32(np.sqrt(0.5))))
            hid[:, cs] = gelu.astype(BF16)
            n_u = ffn // uw
            if u == 0:
                for h in (heads - 2, heads - 1):
                    head_probs(h)
            for h in range(heads):
                if u == min(1 + h * n_u // heads, n_u - 1):
                    value = qkv[:, pl.ds(h * 3 * hd + 2 * hd, hd)]
                    ctx[:, pl.ds(h * hd, hd)] = jnp.dot(probs[h], value, preferred_element_type=F32).astype(BF16)

    def attn_out(c):
        return jnp.dot(ctx[...], wd[:, cols(c)], preferred_element_type=F32)

    def back_chunk(i, c, attn):
        mlp = jnp.dot(hid[...], wdn[:, cols(c)], preferred_element_type=F32)
        attn_next = attn_out(c + 1) if c + 1 < C else None
        psend[lax.rem(i, 2), :, cols(c)] = (mlp + attn).astype(BF16)
        p_copy(i, c).start()
        return attn_next

    lax.fori_loop(0, n_kb, lay_out, 0)
    w_copy(1).start()
    w_copy(2).start()

    def body(i, carry):
        def sums(where):
            here = [c for c in range(C) if SUM_AT[c] == where]
            if here:
                @pl.when(i > 0)
                def _():
                    for c in here:
                        finish_chunk(i - 1, c)

        sums(0)

        @pl.when(is_first)
        def _():
            x_load(i).wait()

        @pl.when(not_first)
        def _():
            for c in range(C):
                f_copy(i, c).wait_recv()

        attention_part(i)

        @pl.when(i == 0)
        def _():
            w_copy(0).wait()

        sums(1)
        up_part(0)
        sums(2)
        up_part(1)

        @pl.when(i == 0)
        def _():
            w_copy(1).wait()
            w_copy(2).wait()

        sums(3)
        attn = attn_out(0)
        for c in range(C):
            attn = back_chunk(i, c, attn)
            sums(4 + c)

        @pl.when(jnp.logical_and(relays, i >= delay))
        def _():
            relay(i - delay)

        return carry

    lax.fori_loop(0, n_micro, body, 0)
    last = n_micro - 1
    for c in range(C):
        finish_chunk(last, c)

    @pl.when(not_last)
    def _():
        for m in (n_micro - 2, n_micro - 1):
            for c in range(C):
                f_copy(m, c).wait_send()

    @pl.when(is_last)
    def _():
        for m in (n_micro - 2, n_micro - 1):
            for c in range(C):
                b_wait(m, c)

    @pl.when(relays)
    def _():
        def more(m, carry):
            relay(m)
            return carry

        lax.fori_loop(jnp.maximum(n_micro - delay, 0), n_micro, more, 0)
        for c in range(C):
            relay_copy(last, c, 0, st - 1).wait_send()

        @pl.when(two_hop)
        def _():
            for c in range(C):
                relay_copy(last, c, 1, 1).wait_send()

    @pl.when(lax.rem(st, 2) == 0)
    def _():
        def leaf(m, carry):
            for c in range(C):
                y_wait(m, c)
            return carry

        lax.fori_loop(0, n_micro, leaf, 0)


def copy_kernel(n, src_hbm, dst_hbm, buf, in_sem, out_sem):
    blk = n // in_sem.shape[0]
    parts = [pl.ds(k * blk, blk) for k in range(n // blk)]
    loads = [pltpu.make_async_copy(src_hbm.at[p], buf.at[p], in_sem.at[k]) for k, p in enumerate(parts)]
    stores = [pltpu.make_async_copy(buf.at[p], dst_hbm.at[p], out_sem.at[k]) for k, p in enumerate(parts)]
    for cp in loads:
        cp.start()
    for load, store in zip(loads, stores):
        load.wait()
    for store in stores:
        store.start()
    for cp in stores:
        cp.wait()


def solution(mesh):
    n_st = mesh.shape["pp"]
    in_specs = (P(), P("pp", None), P("pp", None), P("pp", None, "tp", None), P("pp", "tp", None),
                P("pp", "tp", None, None), P("pp", None), P("pp", None), P("pp", None),
                P("pp", None, "tp"), P("pp", "tp"), P("pp", "tp", None), P("pp", None))

    def device_fn(x_micro, ln1_gain, ln1_bias, w_qkv, b_qkv, w_dense, b_dense, ln2_gain, ln2_bias, w_up, b_up, w_down, b_down):
        n_micro, _, seq, d = x_micro.shape
        heads, hd = w_dense.shape[1], w_dense.shape[2]
        ffn = w_up.shape[2]
        cos_l, sin_lo, sin_hi = rotary_lanes(seq, hd)
        dims = (n_micro, n_st, seq, d, heads, hd, ffn)
        vm = pl.BlockSpec(memory_space=pltpu.VMEM)
        hbm = pl.BlockSpec(memory_space=pl.ANY)
        dma = pltpu.SemaphoreType.DMA
        S, C = X_SLOTS, CHUNKS
        out = pl.pallas_call(
            functools.partial(kernel, dims),
            out_shape=jax.ShapeDtypeStruct((n_micro, seq, d), BF16),
            in_specs=[hbm] + [vm] * 11 + [hbm] * 4,
            out_specs=hbm,
            scratch_shapes=[
                pltpu.VMEM((2, K_BLOCK, heads, 3 * hd), BF16), pltpu.VMEM((3 * hd // 128, K_BLOCK * heads, 128), F32),
                pltpu.VMEM((d, heads * 3 * hd), BF16), pltpu.VMEM((heads * hd, d), BF16),
                pltpu.VMEM((d, ffn), BF16), pltpu.VMEM((ffn, d), BF16),
                pltpu.VMEM((S, seq, d), BF16), pltpu.VMEM((2, seq, d), BF16), pltpu.VMEM((2, seq, d), BF16),
                pltpu.VMEM((2, seq, d), BF16),
                pltpu.VMEM((seq, d), BF16), pltpu.VMEM((seq, d), BF16),
                pltpu.VMEM((seq, heads * 3 * hd), BF16), pltpu.VMEM((heads, seq, seq), BF16), pltpu.VMEM((seq, heads * hd), BF16), pltpu.VMEM((seq, ffn), BF16),
                pltpu.VMEM((1, d), F32), pltpu.VMEM((1, d), F32), pltpu.VMEM((1, d), F32), pltpu.VMEM((1, d), F32),
                pltpu.VMEM((1, heads * 3 * hd), F32), pltpu.VMEM((1, ffn), F32), pltpu.VMEM((1, d), F32),
                dma((3,)), dma((2,)), dma((S,)), dma((S, C)), pltpu.SemaphoreType.REGULAR,
                dma((2, C)), dma((2, C)), dma((2, C)), dma((2, 4, C)), dma((2, C)), dma((n_micro, C)),
            ],
            compiler_params=pltpu.CompilerParams(has_side_effects=True, vmem_limit_bytes=67_043_328),
            name="neox_pipeline",
        )(x_micro.reshape(n_micro, seq, d), jnp.asarray(cos_l), jnp.asarray(sin_lo), jnp.asarray(sin_hi),
          ln1_gain, ln1_bias, ln2_gain, ln2_bias, b_qkv[0], b_up, b_dense, b_down,
          w_qkv[0], w_dense.reshape(heads * hd, d), w_up[0], w_down[0])
        out = pl.pallas_call(functools.partial(copy_kernel, n_micro), out_shape=jax.ShapeDtypeStruct(out.shape, BF16),
                             in_specs=[hbm], out_specs=hbm,
                             scratch_shapes=[pltpu.VMEM(out.shape, BF16), dma((n_micro // 2,)), dma((n_micro // 2,))],
                             compiler_params=pltpu.CompilerParams(vmem_limit_bytes=40_000_000), name="result_copy")(out)
        return out.reshape(x_micro.shape)

    return jax.shard_map(device_fn, mesh=mesh, in_specs=in_specs, out_specs=P(), check_vma=False)
```
